32 devices in a mesh: mem: 8 (over z, x), grid: 4 (over y, core).
Axes of the slice: x: 2, y: 2, z: 4, core: 2. Of those that a mesh axis runs over, the one named last changes fastest.
Arguments:
- alpha: bfloat16 [16, 8, 768, 1536], P('mem', None, 'grid'), may hold values from -6 to 6
- perturbation: bfloat16 [16, 8, 768, 1536], P('mem', None, 'grid'), may hold values from -6 to 6
- legendre: bfloat16 [192, 128, 768], P('grid'), may hold values from -0.21875 to 0.21875
- response: float32 [192, 128], P('grid'), may hold values from 0.2 to 2
Outputs:
- increment: float32 [8, 768, 1536], P('mem', 'grid')
The draws below stay inside these ranges and needn't reach their ends.
All inputs are finite; a program needn't handle non-finite values.
Results may differ from the reference program's by a relative error of at most 0.0063.
Values may be sent and summed in bfloat16 or wider, within the bound.
No kernel may reach another device: no remote copies, remote signals or barrier semaphores. Data moves between devices by JAX's collectives and lax.ppermute only.
A program may use at most 128 MiB of HBM per device.

```python
import math
import jax
import jax.numpy as jnp
from jax import lax

NLON = 1536
NLAT = 768
KEEP = 192
NN = 128
MEMBERS = 16
LEV = 8


def block_scale(stream_key, extent, split, least, top_value):
    def one(axis_at, blocks):
        heights = jax.random.uniform(jax.random.fold_in(jax.random.fold_in(stream_key, 6), axis_at), (blocks,), jnp.float32, least / len(split), top_value / len(split))
        return jnp.repeat(jnp.exp(heights), extent[axis_at] // blocks).reshape((-1,) + (1,) * (len(extent) - axis_at - 1))

    level = one(*split[0])
    for cut in split[1:]:
        level = level * one(*cut)
    return level


def gaussian(stream_key, extent, deviation, most, pieces=(), kind=jnp.bfloat16):
    result = deviation * jax.random.normal(stream_key, extent, jnp.float32)
    if pieces:
        result = result * block_scale(stream_key, extent, pieces, -0.22, 0.18)
    return jnp.clip(result, -most, most).astype(kind)


def setup_inputs(seed: int = 0) -> dict:
    streams_of = jax.random.split(jax.random.key(seed), 5)
    return {
        "alpha": gaussian(streams_of[0], (MEMBERS, LEV, NLAT, NLON), 1.0, 6.0, ((0, 8), (2, 4))),
        "perturbation": gaussian(streams_of[1], (MEMBERS, LEV, NLAT, NLON), 1.0, 6.0, ((0, 8), (2, 4))),
        "legendre": gaussian(streams_of[2], (KEEP, NN, NLAT), NLAT ** -0.5, 0.21875, ((0, 4),)),
        "response": jnp.clip(jnp.exp(math.log(2.0) - 2.3025851 * jax.random.uniform(streams_of[3], (KEEP, NN), jnp.float32) ** block_scale(streams_of[3], (KEEP, NN), ((0, 4),), -0.2, 0.2)), 0.2, 2.0),
    }


def build_tables(lon_count, keep):
    col = jnp.arange(2 * keep, dtype=jnp.int32)
    part = col // keep
    wave = col % keep
    lon = jnp.arange(lon_count, dtype=jnp.int32)
    phase = lon[:, None] * wave[None, :] % lon_count
    angle = phase.astype(jnp.float32) * jnp.float32(2.0 * math.pi / lon_count)
    basis = jnp.where(part[None, :] == 0, jnp.cos(angle), jnp.sin(angle))
    weight = jnp.where(wave == 0, jnp.float32(1.0), jnp.float32(2.0)) / jnp.float32(lon_count)
    forward = basis.astype(jnp.bfloat16)
    inverse = jnp.transpose(basis * weight[None, :]).astype(jnp.bfloat16)
    return (forward, inverse)

def reference(alpha, perturbation, legendre, response):
    members = alpha.shape[0]
    forward, inverse = build_tables(NLON, KEEP)
    legendre_wide = legendre.astype(jnp.float32)

    def one_member(total, pair):
        field, pert = pair
        spec = jnp.dot(field.reshape(LEV * NLAT, NLON), forward, preferred_element_type=jnp.float32)
        spec = spec.astype(jnp.bfloat16).reshape(LEV, NLAT, 2, KEEP)
        coef = jnp.einsum('mnt,ltqm->lqmn', legendre_wide, spec.astype(jnp.float32))
        coef = (coef * response[None, None, :, :]).astype(jnp.bfloat16)
        synth = jnp.einsum('mnt,lqmn->ltqm', legendre_wide, coef.astype(jnp.float32)).astype(jnp.bfloat16)
        values = jnp.dot(synth.reshape(LEV * NLAT, 2 * KEEP), inverse, preferred_element_type=jnp.float32)
        values = values.reshape(LEV, NLAT, NLON)
        return (total + values * pert.astype(jnp.float32), None)
    start = jnp.zeros((LEV, NLAT, NLON), jnp.float32)
    total, unused = lax.scan(one_member, start, (alpha, perturbation))
    return total / jnp.sqrt(jnp.float32(members - 1))
```

```python
import math

import jax
import jax.numpy as jnp
import ml_dtypes
import numpy as np
from jax import lax
from jax.experimental import pallas as pl
from jax.experimental.pallas import tpu as pltpu
from jax.sharding import PartitionSpec as P


def build_tables(lon_count, keep_dev, grid_count):
    col = np.arange(2 * keep_dev * grid_count)
    wave = col // (2 * keep_dev) * keep_dev + col % keep_dev
    part = col // keep_dev % 2
    phase = wave[:, None] * np.arange(lon_count)[None, :] % lon_count
    angle = phase.astype(np.float32) * np.float32(2.0 * math.pi / lon_count)
    basis = np.where(part[:, None] == 0, np.cos(angle), np.sin(angle)).astype(np.float32)
    weight = np.where(wave == 0, np.float32(1.0), np.float32(2.0)) / np.float32(lon_count)
    forward = basis.astype(ml_dtypes.bfloat16)
    inverse = (basis * weight[:, None].astype(np.float32)).astype(ml_dtypes.bfloat16)
    return forward, inverse


def forward_kernel(table, rows, out):
    out[...] = lax.dot_general(
        table[...], rows[...], (((1,), (1,)), ((), ())), preferred_element_type=jnp.float32
    ).astype(out.dtype)


def forward_transform(table, rows):
    count, lon_count = rows.shape
    cols = table.shape[0]
    step = 512 if count % 512 == 0 else 128
    return pl.pallas_call(
        forward_kernel,
        grid=(count // step,),
        in_specs=[
            pl.BlockSpec((cols, lon_count), lambda i: (0, 0)),
            pl.BlockSpec((step, lon_count), lambda i: (i, 0)),
        ],
        out_specs=pl.BlockSpec((cols, step), lambda i: (0, i)),
        out_shape=jax.ShapeDtypeStruct((cols, count), jnp.bfloat16),
        name="forward",
    )(table, rows)


def inverse_kernel(*refs):
    *pieces, table, pert, out = refs
    members, block, lat, lon_count = pert.shape
    lhs = jnp.concatenate([piece[...] for piece in pieces], axis=0)
    total = None
    size = block * lat
    for k in range(members):
        values = lax.dot_general(
            lhs[:, k * size : (k + 1) * size] if size % 128 == 0 else lhs,
            table[...],
            (((0,), (0,)), ((), ())),
            preferred_element_type=jnp.float32,
        )
        if size % 128:
            for j in range(members):
                part = values[j * size : (j + 1) * size] * pert[j].reshape(size, lon_count).astype(jnp.float32)
                total = part if total is None else total + part
            break
        part = values * pert[k].reshape(size, lon_count).astype(jnp.float32)
        total = part if total is None else total + part
    out[...] = total.reshape(block, lat, lon_count).astype(out.dtype)


def inverse_transform(pieces, table, pert, chunk, lat, block):
    members, levels, _, lon_count = pert.shape
    lanes = members * block * lat
    rows = pieces[0].shape[0]
    return pl.pallas_call(
        inverse_kernel,
        grid=(levels // block,),
        in_specs=[pl.BlockSpec((rows, lanes), lambda i: (0, i)) for _ in pieces]
        + [
            pl.BlockSpec(table.shape, lambda i: (0, 0)),
            pl.BlockSpec((members, block, lat, lon_count), lambda i: (0, i, chunk, 0)),
        ],
        out_specs=pl.BlockSpec((block, lat, lon_count), lambda i: (i, 0, 0)),
        out_shape=jax.ShapeDtypeStruct((levels, lat, lon_count), jnp.bfloat16),
        name="inverse",
    )(*pieces, table, pert)


def swap(value, axis, shift):
    count = lax.axis_size(axis)
    return lax.ppermute(value, axis, [(a, a ^ shift) for a in range(count)])


def pick(value, index, axis=0):
    return lax.dynamic_index_in_dim(value, index, axis, keepdims=False)


def body(alpha, perturbation, legendre, response):
    members, levels, lat_dev, lon_count = alpha.shape
    keep_dev = legendre.shape[0]
    grid_count = lax.axis_size("grid")
    mem_count = lax.axis_size("mem")
    chunks = next(c for c in (4, 2, 1) if lat_dev % (16 * c) == 0)
    lat = lat_dev // chunks
    block = next(b for b in (1, 2, 4, 8, 16) if members * b * lat % 128 == 0)
    cols = 2 * keep_dev
    here = lax.axis_index("grid")
    mine = lax.axis_index("mem")
    forward, inverse = build_tables(lon_count, keep_dev, grid_count)
    spectra = forward_transform(jnp.asarray(forward), alpha.reshape(-1, lon_count))
    spectra = spectra.reshape(grid_count, cols, members * levels * lat_dev)
    spectra = lax.all_to_all(spectra, "grid", 0, 0, tiled=True)
    split = spectra.reshape(grid_count, 2, keep_dev, members, levels, lat_dev)
    split = split.transpose(1, 2, 3, 4, 0, 5).reshape(2, keep_dev, members, levels, -1)
    coef = jnp.einsum("mnt,qmkit->qmkin", legendre, split, preferred_element_type=jnp.float32)
    coef = (coef * response[None, :, None, None, :]).astype(jnp.bfloat16)
    synth = jnp.einsum("mnt,qmkin->qmkit", legendre, coef, preferred_element_type=jnp.float32)
    synth = synth.astype(jnp.bfloat16)
    synth = synth.reshape(cols, members, levels // block, block, grid_count, chunks, lat)
    synth = synth.transpose(4, 5, 0, 2, 1, 3, 6).reshape(grid_count, chunks, cols, -1)
    order = [here ^ s for s in range(grid_count)]
    table = jnp.asarray(inverse).reshape(grid_count, cols, lon_count)
    table = jnp.concatenate([pick(table, o) for o in order], axis=0)
    sends = [pick(synth, o) for o in order]
    low = mine % 2
    high = mine // 2
    scale = 1.0 / jnp.sqrt(jnp.float32(members * mem_count - 1))
    results = []
    for j in range(chunks):
        pieces = [sends[0][j]] + [swap(sends[s][j], "grid", s) for s in range(1, grid_count)]
        part = inverse_transform(pieces, table, perturbation, j, lat, block)
        part = part.reshape(mem_count // 2, 2, levels // mem_count, lat, lon_count)
        got = swap(pick(part, 1 - low, 1), "mem", 1)
        half = pick(part, low, 1).astype(jnp.float32) + got.astype(jnp.float32)
        half = half.astype(jnp.bfloat16)
        total = pick(half, high).astype(jnp.float32)
        for s in range(1, mem_count // 2):
            total = total + swap(pick(half, high ^ s), "mem", 2 * s).astype(jnp.float32)
        results.append(total * scale)
    return jnp.concatenate(results, axis=1)


def solution(mesh):
    placed = (
        P("mem", None, "grid", None),
        P("mem", None, "grid", None),
        P("grid", None, None),
        P("grid", None),
    )
    return jax.shard_map(
        body, mesh=mesh, in_specs=placed, out_specs=P("mem", "grid", None), check_vma=False
    )
```

```python
import functools
import math

import jax
import jax.numpy as jnp
import ml_dtypes
import numpy as np
from jax import lax
from jax.experimental import pallas as pl
from jax.experimental.pallas import tpu as pltpu
from jax.sharding import PartitionSpec as P


def build_tables(lon_count, keep_dev, grid_count):
    col = np.arange(2 * keep_dev * grid_count)
    wave = col // (2 * keep_dev) * keep_dev + col % keep_dev
    part = col // keep_dev % 2
    phase = wave[:, None] * np.arange(lon_count)[None, :] % lon_count
    angle = phase.astype(np.float32) * np.float32(2.0 * math.pi / lon_count)
    basis = np.where(part[:, None] == 0, np.cos(angle), np.sin(angle)).astype(np.float32)
    weight = np.where(wave == 0, np.float32(1.0), np.float32(2.0)) / np.float32(lon_count)
    forward = basis.astype(ml_dtypes.bfloat16)
    inverse = (basis * weight[:, None].astype(np.float32)).astype(ml_dtypes.bfloat16)
    return forward, inverse


def forward_kernel(table, rows, out):
    out[...] = lax.dot_general(
        table[...], rows[...], (((1,), (1,)), ((), ())), preferred_element_type=jnp.float32
    ).astype(out.dtype)


def forward_transform(table, rows):
    count, lon_count = rows.shape
    cols = table.shape[0]
    step = 512 if count % 512 == 0 else 128
    return pl.pallas_call(
        forward_kernel,
        grid=(count // step,),
        in_specs=[
            pl.BlockSpec((cols, lon_count), lambda i: (0, 0)),
            pl.BlockSpec((step, lon_count), lambda i: (i, 0)),
        ],
        out_specs=pl.BlockSpec((cols, step), lambda i: (0, i)),
        out_shape=jax.ShapeDtypeStruct((cols, count), jnp.bfloat16),
        name="forward",
    )(table, rows)


def inverse_kernel(*refs):
    *pieces, table, pert, out = refs
    members, block, lat, lon_count = pert.shape
    lhs = jnp.concatenate([piece[...] for piece in pieces], axis=0)
    total = None
    size = block * lat
    for k in range(members):
        values = lax.dot_general(
            lhs[:, k * size : (k + 1) * size] if size % 128 == 0 else lhs,
            table[...],
            (((0,), (0,)), ((), ())),
            preferred_element_type=jnp.float32,
        )
        if size % 128:
            for j in range(members):
                part = values[j * size : (j + 1) * size] * pert[j].reshape(size, lon_count).astype(jnp.float32)
                total = part if total is None else total + part
            break
        part = values * pert[k].reshape(size, lon_count).astype(jnp.float32)
        total = part if total is None else total + part
    out[...] = total.reshape(block, lat, lon_count).astype(out.dtype)


def inverse_transform(pieces, table, pert, chunk, lat, block):
    members, levels, _, lon_count = pert.shape
    lanes = members * block * lat
    rows = pieces[0].shape[0]
    return pl.pallas_call(
        inverse_kernel,
        grid=(levels // block,),
        in_specs=[pl.BlockSpec((rows, lanes), lambda i: (0, i)) for _ in pieces]
        + [
            pl.BlockSpec(table.shape, lambda i: (0, 0)),
            pl.BlockSpec((members, block, lat, lon_count), lambda i: (0, i, chunk, 0)),
        ],
        out_specs=pl.BlockSpec((block, lat, lon_count), lambda i: (i, 0, 0)),
        out_shape=jax.ShapeDtypeStruct((levels, lat, lon_count), jnp.bfloat16),
        name="inverse",
    )(*pieces, table, pert)


def legendre_kernel(block, here, spectra, legendre, response, out, before, after):
    grid_count, parts, waves, _ = spectra.shape
    chunks, lanes = out.shape[1], out.shape[4]
    items = before.shape[0] // parts
    lat_dev = spectra.shape[3] // items
    lat = lat_dev // chunks
    levels = items // 2
    for q in range(parts):
        for i in range(items):
            rows = [spectra[s, q, :, i * lat_dev : (i + 1) * lat_dev] for s in range(grid_count)]
            before[q * items + i] = jnp.concatenate([r.astype(jnp.float32) for r in rows], axis=1)
    for m in range(waves):
        matrix = legendre[m]
        coef = lax.dot_general(
            before[:, m, :].astype(jnp.bfloat16),
            matrix,
            (((1,), (1,)), ((), ())),
            preferred_element_type=jnp.float32,
        )
        coef = (coef * response[m : m + 1, :]).astype(jnp.bfloat16)
        after[:, m, :] = jnp.dot(coef, matrix, preferred_element_type=jnp.float32)
    for q in range(parts):
        for i in range(items):
            k, l = i // levels, i % levels
            at = ((l // block * 2 + k) * block + l % block) * lat
            for s in range(grid_count):
                slot = lax.bitwise_xor(here[0], s)
                for j in range(chunks):
                    start = s * lat_dev + j * lat
                    out[slot, j, q, :, at : at + lat] = after[q * items + i, :, start : start + lat].astype(out.dtype)


def legendre_filter(here, spectra, legendre, response, items, chunks, block):
    grid_count, cols, lanes = spectra.shape
    keep_dev, degrees, lat_count = legendre.shape
    waves = 16
    spectra = spectra.reshape(grid_count, 2, keep_dev, lanes)
    out = pl.pallas_call(
        functools.partial(legendre_kernel, block),
        grid_spec=pltpu.PrefetchScalarGridSpec(
            num_scalar_prefetch=1,
            grid=(keep_dev // waves,),
            in_specs=[
                pl.BlockSpec((grid_count, 2, waves, lanes), lambda i, h: (0, 0, i, 0)),
                pl.BlockSpec((waves, degrees, lat_count), lambda i, h: (i, 0, 0)),
                pl.BlockSpec((waves, degrees), lambda i, h: (i, 0)),
            ],
            out_specs=pl.BlockSpec(
                (grid_count, chunks, 2, waves, lanes // chunks), lambda i, h: (0, 0, 0, i, 0)
            ),
            scratch_shapes=[pltpu.VMEM((2 * items, waves, lat_count), jnp.float32)] * 2,
        ),
        out_shape=jax.ShapeDtypeStruct(
            (grid_count, chunks, 2, keep_dev, lanes // chunks), jnp.bfloat16
        ),
        name="legendre",
    )(here.reshape(1).astype(jnp.int32), spectra, legendre, response)
    return out.reshape(grid_count, chunks, cols, lanes // chunks)


def swap(value, axis, shift):
    count = lax.axis_size(axis)
    return lax.ppermute(value, axis, [(a, a ^ shift) for a in range(count)])


def pick(value, index, axis=0):
    return lax.dynamic_index_in_dim(value, index, axis, keepdims=False)


def legendre_plain(spectra, legendre, response, members, levels, lat_dev, block, chunks):
    grid_count, cols, _ = spectra.shape
    keep_dev = legendre.shape[0]
    lat = lat_dev // chunks
    split = spectra.reshape(grid_count, 2, keep_dev, members, levels, lat_dev)
    split = split.transpose(1, 2, 3, 4, 0, 5).reshape(2, keep_dev, members, levels, -1)
    coef = jnp.einsum("mnt,qmkit->qmkin", legendre, split, preferred_element_type=jnp.float32)
    coef = (coef * response[None, :, None, None, :]).astype(jnp.bfloat16)
    synth = jnp.einsum("mnt,qmkin->qmkit", legendre, coef, preferred_element_type=jnp.float32)
    synth = synth.astype(jnp.bfloat16)
    synth = synth.reshape(cols, members, levels // block, block, grid_count, chunks, lat)
    synth = synth.transpose(4, 5, 0, 2, 1, 3, 6).reshape(grid_count, chunks, cols, -1)
    return synth


def body(alpha, perturbation, legendre, response):
    members, levels, lat_dev, lon_count = alpha.shape
    keep_dev = legendre.shape[0]
    grid_count = lax.axis_size("grid")
    mem_count = lax.axis_size("mem")
    chunks = next(c for c in (4, 2, 1) if lat_dev % (16 * c) == 0)
    lat = lat_dev // chunks
    block = next(b for b in (1, 2, 4, 8, 16) if members * b * lat % 128 == 0)
    cols = 2 * keep_dev
    here = lax.axis_index("grid")
    mine = lax.axis_index("mem")
    forward, inverse = build_tables(lon_count, keep_dev, grid_count)
    spectra = forward_transform(jnp.asarray(forward), alpha.reshape(-1, lon_count))
    spectra = spectra.reshape(grid_count, cols, members * levels * lat_dev)
    spectra = lax.all_to_all(spectra, "grid", 0, 0, tiled=True)
    order = [here ^ s for s in range(grid_count)]
    if keep_dev % 16 == 0 and members == 2:
        sends = legendre_filter(here, spectra, legendre, response, members * levels, chunks, block)
    else:
        synth = legendre_plain(spectra, legendre, response, members, levels, lat_dev, block, chunks)
        sends = jnp.stack([pick(synth, o) for o in order])
    table = jnp.asarray(inverse).reshape(grid_count, cols, lon_count)
    table = jnp.concatenate([pick(table, o) for o in order], axis=0)
    low = mine % 2
    high = mine // 2
    scale = 1.0 / jnp.sqrt(jnp.float32(members * mem_count - 1))
    results = []
    for j in range(chunks):
        pieces = [sends[0][j]] + [swap(sends[s][j], "grid", s) for s in range(1, grid_count)]
        part = inverse_transform(pieces, table, perturbation, j, lat, block)
        part = part.reshape(mem_count // 2, 2, levels // mem_count, lat, lon_count)
        got = swap(pick(part, 1 - low, 1), "mem", 1)
        half = pick(part, low, 1).astype(jnp.float32) + got.astype(jnp.float32)
        half = half.astype(jnp.bfloat16)
        total = pick(half, high).astype(jnp.float32)
        for s in range(1, mem_count // 2):
            total = total + swap(pick(half, high ^ s), "mem", 2 * s).astype(jnp.float32)
        results.append(total * scale)
    return jnp.concatenate(results, axis=1)


def solution(mesh):
    placed = (
        P("mem", None, "grid", None),
        P("mem", None, "grid", None),
        P("grid", None, None),
        P("grid", None),
    )
    return jax.shard_map(
        body, mesh=mesh, in_specs=placed, out_specs=P("mem", "grid", None), check_vma=False
    )
```
